256 devices in a mesh: ctx: 64 (over z_lo, y, x, core), head: 4 (over z_hi).
Axes of the slice: x: 4, y: 4, z: 8 (z_hi: 4, z_lo: 2; z = z_hi * 2 + z_lo), core: 2. Of those that a mesh axis runs over, the one named last changes fastest.
Arguments:
- queries: bfloat16 [12288, 4096], P('ctx', 'head'), may hold values from -6 to 6
- keys: bfloat16 [12288, 1024], P('ctx', 'head'), may hold values from -6 to 6
- values: bfloat16 [12288, 1024], P('ctx', 'head'), may hold values from -6 to 6
- retrieval: int32 [32], replicated, may hold values 0 or 1
- spans: int32 [2, 32], replicated, may hold values from 64 to 4096, as said below
- out_weight: bfloat16 [4096, 4096], P(None, 'head'), may hold values from -0.09375 to 0.09375
Outputs:
- layer_out: bfloat16 [12288, 4096], P('ctx', 'head')
The draws below stay inside these ranges and needn't reach their ends.
Inputs may be any that keep to these rules, and one draw needn't show every extreme that they name: `spans`: row 0 lies within 64 to 128, row 1 within 2048 to 4096; some head has exactly 128 sink tokens and some head exactly 4096 recent tokens.
All inputs are finite; a program needn't handle non-finite values.
Results may differ from the reference program's by a relative error of at most 0.0075.
Values may be sent and summed in bfloat16 or wider, within the bound.
No kernel may reach another device: no remote copies, remote signals or barrier semaphores. Data moves between devices by JAX's collectives and lax.ppermute only.
A program may use at most 192 MiB of HBM per device.

```python
import jax
import jax.numpy as jnp
from jax import lax

D = 4096
QH = 32
KVH = 8
HD = 128
TOK_DEV = 192
SINK = 128
WINDOW = 4096
SEQ = 12288
N_CTX = 64


def draw_queries(key, part):
    drawn = jnp.clip(jax.random.normal(jax.random.fold_in(key, 11), (SEQ, QH * HD), jnp.float32), -6.0, 6.0)
    return drawn.astype(jnp.bfloat16)


def draw_keys(key, part):
    drawn = jnp.clip(jax.random.normal(jax.random.fold_in(key, 12), (SEQ, KVH * HD), jnp.float32), -6.0, 6.0)
    return drawn.astype(jnp.bfloat16)


def draw_spans(key, part):
    sink_sizes = jax.random.randint(jax.random.fold_in(key, 21), (QH,), SINK // 2, SINK + 1)
    window_sizes = jax.random.randint(jax.random.fold_in(key, 22), (QH,), WINDOW // 2, WINDOW + 1)
    picked = jax.random.randint(jax.random.fold_in(key, 23), (2,), 0, QH)
    sink_sizes = sink_sizes.at[picked[0]].set(SINK)
    window_sizes = window_sizes.at[picked[1]].set(WINDOW)
    return jnp.stack([sink_sizes, window_sizes]).astype(jnp.int32)


def place_ends(values, stream_key, least, high):
    extent = values.shape
    place = [jax.random.randint(jax.random.fold_in(stream_key, axis), (), 0, extent[axis]) for axis in range(len(extent))]
    values = values.at[tuple(place)].set(least)
    longest = extent.index(max(extent))
    place[longest] = (place[longest] + 1) % extent[longest]
    return values.at[tuple(place)].set(high)


def block_scale(own_key, extent, split, smallest, high):
    def one(position, blocks):
        heights = jax.random.uniform(jax.random.fold_in(jax.random.fold_in(own_key, 6), position), (blocks,), jnp.float32, smallest / len(split), high / len(split))
        return jnp.repeat(jnp.exp(heights), extent[position] // blocks).reshape((-1,) + (1,) * (len(extent) - position - 1))

    loudness = one(*split[0])
    for cut in split[1:]:
        loudness = loudness * one(*cut)
    return loudness


def scatter_about(stream_key, dims, width, bound, cuts=(), held_as=jnp.bfloat16):
    drawn = jax.random.normal(stream_key, dims, jnp.float32) * width
    if len(cuts) > 0:
        drawn = block_scale(stream_key, dims, cuts, -0.22, 0.18) * drawn
    return jnp.clip(drawn, min=-bound, max=bound).astype(held_as)


def setup_inputs(seed: int = 0) -> dict:
    streams_of = jax.random.split(jax.random.key(seed), 7)
    queries = draw_queries(jax.random.fold_in(streams_of[6], 71), 0)
    keys = draw_keys(jax.random.fold_in(streams_of[6], 71), 0)
    values = scatter_about(streams_of[2], (SEQ, KVH * HD), 1.0, 6.0, ((0, 64), (1, 4)))
    retrieval = place_ends((jax.random.randint(streams_of[3], (QH,), 0, 2) < 1).astype(jnp.int32), jax.random.fold_in(streams_of[3], 1), 0, 1)
    spans = draw_spans(jax.random.fold_in(streams_of[6], 71), 0)
    out_weight = scatter_about(streams_of[5], (D, D), D ** -0.5, 0.09375, ((1, 4),))
    return dict(queries=queries, keys=keys, values=values, retrieval=retrieval, spans=spans, out_weight=out_weight)


def attend_block(queries_block, offset, keys, values, retrieval, spans):
    row_count = queries_block.shape[0]
    group_size = QH // KVH
    query_heads = queries_block.reshape(row_count, KVH, group_size, HD).astype(jnp.float32)
    key_heads = keys.reshape(SEQ, KVH, HD).astype(jnp.float32)
    value_heads = values.reshape(SEQ, KVH, HD).astype(jnp.float32)
    scores = jnp.einsum("qgjd,kgd->qgjk", query_heads, key_heads) * (HD ** -0.5)
    query_pos = offset + jnp.arange(row_count, dtype=jnp.int32)
    key_pos = jnp.arange(SEQ, dtype=jnp.int32)
    retrieval_heads = retrieval.reshape(KVH, group_size) > 0
    sink_sizes = spans[0].reshape(KVH, group_size)
    window_sizes = spans[1].reshape(KVH, group_size)
    gap = query_pos[:, None] - key_pos[None, :]
    reach = retrieval_heads[None, :, :, None] | (key_pos[None, None, None, :] < sink_sizes[None, :, :, None])
    reach = reach | (gap[:, None, None, :] < window_sizes[None, :, :, None])
    allowed = (gap >= 0)[:, None, None, :] & reach
    masked = jnp.where(allowed, scores, -1e30)
    peaks = jnp.max(masked, axis=-1, keepdims=True)
    weights = jnp.where(allowed, jnp.exp(masked - peaks), 0.0)
    totals = jnp.sum(weights, axis=-1)
    rounded = lax.optimization_barrier(weights.astype(jnp.bfloat16)).astype(jnp.float32)
    mixed = jnp.einsum("qgjk,kgd->qgjd", rounded, value_heads) / totals[..., None]
    return mixed.reshape(row_count, QH * HD).astype(jnp.bfloat16)


def reference(queries, keys, values, retrieval, spans, out_weight):
    blocks = queries.reshape(N_CTX, TOK_DEV, QH * HD)
    offsets = jnp.arange(N_CTX, dtype=jnp.int32) * TOK_DEV

    def one_block(pair):
        return attend_block(pair[0], pair[1], keys, values, retrieval, spans)

    attended = lax.map(one_block, (blocks, offsets)).reshape(SEQ, QH * HD)
    return jnp.dot(attended, out_weight, preferred_element_type=jnp.float32).astype(jnp.bfloat16)
```

```python
import functools

import jax
import jax.numpy as jnp
from jax import lax
from jax.experimental import pallas as pl
from jax.experimental.pallas import tpu as pltpu
from jax.sharding import PartitionSpec as P

HD = 128
ROWS = 192
SEQ = 12288
TILE = 768
SINK = 128
GROUP = 4
NEG = -1e30


def ctx_pairs(flip):
    return [(i, i ^ flip) for i in range(64)]


CORE = ctx_pairs(1)
X1, X3 = ctx_pairs(1 * 2), ctx_pairs(3 * 2)
Y1, Y3 = ctx_pairs(1 * 8), ctx_pairs(3 * 8)
Z1 = ctx_pairs(32)
H1 = [(i, i ^ 1) for i in range(4)]
H3 = [(i, i ^ 3) for i in range(4)]
STREAMS = (
    ((X1, X3, Y1, Y3), (1, 3), (1, 3), False),
    ((Y1, Y3, X1, X3), (1, 3), (1, 3), True),
    ((X3, X1, Y3, Y1), (3, 1), (3, 1), False),
    ((Y3, Y1, X3, X1), (3, 1), (3, 1), True),
)


def swap(a, pairs):
    return lax.ppermute(a, "ctx", pairs)


def attention_kernel(info, qm, qr, *refs):
    pieces, (om, orr, kbuf, vbuf, qbuf, obuf, acc, top, tot, sems) = refs[:16], refs[16:]
    pos, half = info[12], info[13]
    y, x, core = pos // 8, (pos // 2) % 4, pos % 2

    copies = []
    for s in range(4):
        _, f1, f2, y_first = STREAMS[s]
        dst = kbuf if s < 2 else vbuf
        z = s % 2
        for part in range(4):
            src = pieces[s * 4 + part]
            i4, other = part % 2, part // 2
            for e in range(8):
                i1, i2, i3 = e % 2, (e // 2) % 2, e // 4
                a = (f1[0] * i1) ^ (f1[1] * i2)
                b = (f2[0] * i3) ^ (f2[1] * i4)
                fx, fy = (b, a) if y_first else (a, b)
                block = z * 32 + (y ^ fy) * 8 + (x ^ fx) * 2 + (core ^ other)
                copies.append(
                    pltpu.make_async_copy(
                        src.at[e], dst.at[pl.ds(block * ROWS, ROWS)], sems.at[s * 4 + part]
                    )
                )
    for c in copies:
        c.start()
    for j in range(GROUP):
        qbuf[j] = qm[:, j * HD : (j + 1) * HD]
        qbuf[GROUP + j] = qr[:, j * HD : (j + 1) * HD]
    for c in copies:
        c.wait()

    factor = HD ** (-0.5) * 1.4426950408889634

    def absorb(q, keys, values, mask, first):
        s = lax.dot_general(q, keys, (((1,), (1,)), ((), ())), preferred_element_type=jnp.float32)
        s = s * factor
        if mask is not None:
            s = jnp.where(mask, s, NEG)
        high = jnp.max(s, axis=1, keepdims=True)
        old = top[:, :1]
        new = jnp.maximum(old, high)
        p = jnp.exp2(s - new)
        fade = jnp.exp2(old - new)
        part = p[:, :HD]
        for n in range(1, p.shape[1] // HD):
            part = part + p[:, n * HD : (n + 1) * HD]
        tot[...] = tot[...] * fade + part
        pv = jnp.dot(p.astype(jnp.bfloat16), values, preferred_element_type=jnp.float32)
        acc[...] = acc[...] * fade + pv
        top[...] = jnp.broadcast_to(new, top.shape)

    def unit(u, _):
        j, far = u % GROUP, u // GROUP
        z = jnp.where(far == 1, 1 - half, half)
        block = z * 32 + pos
        row0 = block * ROWS
        keep, sink, win = info[j], info[4 + j], info[8 + j]
        reach = jnp.where(keep > 0, SEQ + ROWS, win)
        first_key = jnp.maximum(row0 - reach + 1, 0)
        lo = first_key // TILE
        diag = row0 // TILE
        q = qbuf[u]
        acc[...] = jnp.zeros_like(acc)
        tot[...] = jnp.zeros_like(tot)
        top[...] = jnp.full_like(top, NEG)

        @pl.when(lo > 0)
        def _():
            col = lax.broadcasted_iota(jnp.int32, (ROWS, SINK), 1)
            absorb(q, kbuf[:SINK], vbuf[:SINK], col < sink, True)

        def tile(t, _):
            start = t * TILE
            keys = kbuf.at[pl.ds(pl.multiple_of(start, TILE), TILE)]
            values = vbuf.at[pl.ds(pl.multiple_of(start, TILE), TILE)]
            edge = (t == diag) | (start < row0 + ROWS - reach)

            @pl.when(edge)
            def _():
                col = start + lax.broadcasted_iota(jnp.int32, (ROWS, TILE), 1)
                row = row0 + lax.broadcasted_iota(jnp.int32, (ROWS, TILE), 0)
                gap = row - col
                mask = (gap >= 0) & ((gap < reach) | (col < sink))
                absorb(q, keys[...], values[...], mask, False)

            @pl.when(jnp.logical_not(edge))
            def _():
                absorb(q, keys[...], values[...], None, False)

            return 0

        lax.fori_loop(lo, diag + 1, tile, 0)
        total = jnp.sum(tot[...], axis=1, keepdims=True)
        obuf[u] = (acc[...] / total).astype(jnp.bfloat16)
        return 0

    lax.fori_loop(0, 2 * GROUP, unit, 0)
    for j in range(GROUP):
        om[:, j * HD : (j + 1) * HD] = obuf[j]
        orr[:, j * HD : (j + 1) * HD] = obuf[GROUP + j]


def attention(info, q_mine, q_other, pieces):
    out = jax.ShapeDtypeStruct((ROWS, GROUP * HD), jnp.bfloat16)
    vmem = pl.BlockSpec(memory_space=pltpu.VMEM)
    return pl.pallas_call(
        attention_kernel,
        out_shape=(out, out),
        in_specs=[pl.BlockSpec(memory_space=pltpu.SMEM), vmem, vmem]
        + [pl.BlockSpec(memory_space=pl.ANY)] * 16,
        out_specs=(vmem, vmem),
        scratch_shapes=[
            pltpu.VMEM((SEQ, HD), jnp.bfloat16),
            pltpu.VMEM((SEQ, HD), jnp.bfloat16),
            pltpu.VMEM((2 * GROUP, ROWS, HD), jnp.bfloat16),
            pltpu.VMEM((2 * GROUP, ROWS, HD), jnp.bfloat16),
            pltpu.VMEM((ROWS, HD), jnp.float32),
            pltpu.VMEM((ROWS, HD), jnp.float32),
            pltpu.VMEM((ROWS, HD), jnp.float32),
            pltpu.SemaphoreType.DMA((16,)),
        ],
        compiler_params=pltpu.CompilerParams(vmem_limit_bytes=24 * 2**20),
        cost_estimate=pl.CostEstimate(
            flops=7_000_000_000, bytes_accessed=8_000_000, transcendentals=14_000_000
        ),
    )(info, q_mine, q_other, *pieces)


def project_kernel(info, a0, a1, a2, b0, b1, b2, w, out):
    h, z = info[14], info[13]
    width = GROUP * HD

    def term(ref, piece, group, kv):
        start = pl.multiple_of((2 * group + kv) * width, width)
        return jnp.dot(piece, w[pl.ds(start, width)], preferred_element_type=jnp.float32)

    total = term(a0, a0[...], h, z)
    total += term(b0, b0[...], h, 1 - z)
    total += term(a1, a1[...], h ^ 1, z)
    total += term(b1, b1[...], h ^ 3, 1 - z)
    total += term(a2, a2[0], h ^ 3, z)
    total += term(a2, a2[1], h ^ 2, z)
    total += term(b2, b2[0], h ^ 1, 1 - z)
    total += term(b2, b2[1], h ^ 2, 1 - z)
    out[...] = total.astype(out.dtype)


def project(info, pieces, w):
    vmem = pl.BlockSpec(memory_space=pltpu.VMEM)
    return pl.pallas_call(
        project_kernel,
        out_shape=jax.ShapeDtypeStruct((ROWS, w.shape[1]), jnp.bfloat16),
        in_specs=[pl.BlockSpec(memory_space=pltpu.SMEM)] + [vmem] * 7,
        out_specs=vmem,
        compiler_params=pltpu.CompilerParams(vmem_limit_bytes=24 * 2**20),
    )(info, *pieces, w)


def body(queries, keys, values, retrieval, spans, out_weight):
    at = lax.axis_index("ctx")
    h = lax.axis_index("head")
    half, pos = at // 32, at % 32
    width = GROUP * HD
    kv_both = jnp.stack([keys, values])
    kv_mine = lax.dynamic_slice_in_dim(kv_both, half * HD, HD, axis=2)
    kv_out = lax.dynamic_slice_in_dim(kv_both, (1 - half) * HD, HD, axis=2)
    q_mine = lax.dynamic_slice_in_dim(queries, half * width, width, axis=1)
    q_out = lax.dynamic_slice_in_dim(queries, (1 - half) * width, width, axis=1)
    kv_in = swap(kv_out, Z1)
    q_in = swap(q_out, Z1)
    first = (2 * h + half) * GROUP
    mine = lambda a: lax.dynamic_slice_in_dim(a, first, GROUP)
    info = jnp.concatenate(
        [
            mine(retrieval),
            mine(spans[0]),
            mine(spans[1]),
            jnp.stack([pos, half, h, jnp.int32(0)]),
        ]
    )
    low = jnp.where(half == 0, kv_mine, kv_in)
    high = jnp.where(half == 0, kv_in, kv_mine)
    held = [low[0][None], high[0][None], low[1][None], high[1][None]]
    for step in range(3):
        got = [swap(held[s], STREAMS[s][0][step]) for s in range(4)]
        held = [jnp.concatenate([a, b]) for a, b in zip(held, got)]
    last = [swap(held[s], STREAMS[s][0][3]) for s in range(4)]
    held_other = [swap(a, CORE) for a in held]
    last_other = [swap(a, CORE) for a in last]
    pieces = []
    for s in range(4):
        pieces += [held[s], last[s], held_other[s], last_other[s]]
    att_mine, att_other = attention(info, q_mine, q_in, pieces)

    partner = swap(att_other, Z1)
    a1 = lax.ppermute(att_mine, "head", H1)
    b1 = lax.ppermute(partner, "head", H3)
    a2 = lax.ppermute(jnp.stack([att_mine, a1]), "head", H3)
    b2 = lax.ppermute(jnp.stack([partner, b1]), "head", H1)
    return project(info, (att_mine, a1, a2, partner, b1, b2), out_weight)


def solution(mesh):
    in_specs = (P("ctx", "head"), P("ctx", "head"), P("ctx", "head"), P(), P(), P(None, "head"))
    out_specs = P("ctx", "head")
    return jax.shard_map(body, mesh=mesh, in_specs=in_specs, out_specs=out_specs, check_vma=False)
```

```python
import functools

import jax
import jax.numpy as jnp
from jax import lax
from jax.experimental import pallas as pl
from jax.experimental.pallas import tpu as pltpu
from jax.sharding import PartitionSpec as P

HD = 128
ROWS = 192
SEQ = 12288
TILE = 768
TILES = SEQ // TILE
STRIP = 32
GROUP = 4
NEG = -1e30


def ctx_pairs(flip):
    return [(i, i ^ flip) for i in range(64)]


def by_core(flip0, flip1):
    return [(i, i ^ (flip1 if i % 2 else flip0)) for i in range(64)]


def to_class(turn):
    return [(i, ((i % 2) ^ turn) * 32 + (i % 32) // 2 * 2 + i // 32) for i in range(64)]


CORE = ctx_pairs(1)
MIRROR = ctx_pairs(63)
KEY_STEPS = (by_core(2, 8), by_core(6, 24), by_core(8, 2), by_core(24, 6))
VALUE_STEPS = (KEY_STEPS[1], KEY_STEPS[0], KEY_STEPS[3], KEY_STEPS[2])
H1 = [(i, i ^ 1) for i in range(4)]
H3 = [(i, i ^ 3) for i in range(4)]


def swap(a, pairs):
    return lax.ppermute(a, "ctx", pairs)


def attention_kernel(info, qm, qr, *refs):
    pieces, (om, orr), scratch = refs[:8], refs[8:10], refs[10:]
    kbuf, vbuf, qbuf, acc, top, tot, gaps, sa, sb, pa, pb, fa, fb, items = scratch
    pos, half = info[12], info[13]
    y, x, core = pos // 8, (pos // 2) % 4, pos % 2

    for s in range(8):
        value, other, late = s // 4, (s // 2) % 2, s % 2
        dst = vbuf if value else kbuf
        f1, f3 = (3, 1) if value else (1, 3)
        z = core ^ other
        for e in range(16):
            a = (f1 * ((e // 2) % 2)) ^ (f3 * ((e // 4) % 2))
            b = (f1 * (e // 8)) ^ (f3 * late)
            fx, fy = jnp.where(z == 0, a, b), jnp.where(z == 0, b, a)
            block = z * 32 + (y ^ fy) * 8 + (x ^ fx) * 2 + (half ^ (e % 2))
            dst[pl.ds(pl.multiple_of(block * ROWS, ROWS), ROWS)] = pieces[s][e]
    for j in range(GROUP):
        qbuf[j] = qm[:, j * HD : (j + 1) * HD]
        qbuf[GROUP + j] = qr[:, j * HD : (j + 1) * HD]
    acc[...] = jnp.zeros_like(acc)
    tot[...] = jnp.zeros_like(tot)
    top[...] = jnp.full_like(top, NEG)
    gaps[...] = lax.broadcasted_iota(jnp.int32, gaps.shape, 0) - lax.broadcasted_iota(
        jnp.int32, gaps.shape, 1
    )

    def row_of(u):
        at = half * 32 + pos
        return jnp.where(u // GROUP == 1, 63 - at, at) * ROWS

    def reach_of(u):
        j = u % GROUP
        return jnp.where(info[j] > 0, SEQ + ROWS, info[8 + j])

    def list_unit(u, counts):
        row0, reach = row_of(u), reach_of(u)
        low = jnp.maximum(row0 - reach + 1, 0) // TILE
        diag = row0 // TILE

        def put(t, counts):
            edge = (t == diag) | (t * TILE < row0 + ROWS - reach)
            kind = jnp.where(edge, 0, 1)
            n = jnp.where(edge, counts[0], counts[1])
            items[kind, n] = u * TILES + t
            return counts[0] + 1 - kind, counts[1] + kind

        counts = lax.cond(low > 0, lambda c: put(0, c), lambda c: c, counts)
        return lax.fori_loop(low, diag + 1, put, counts)

    masked, plain = lax.fori_loop(0, 2 * GROUP, list_unit, (0, 0))
    odd = plain % 2
    items[0, masked] = items[1, jnp.maximum(plain - 1, 0)]
    masked, plain = masked + odd, plain - odd
    items[0, masked] = items[0, 0]
    items[0, masked + 1] = items[0, 0]
    items[1, plain] = 0

    factor = HD ** (-0.5) * 1.4426950408889634

    def span(t):
        return pl.ds(pl.multiple_of(t * TILE, TILE), TILE)

    def score(item, s_ref):
        s_ref[...] = lax.dot_general(
            qbuf[item // TILES],
            kbuf[span(item % TILES)],
            (((1,), (1,)), ((), ())),
            preferred_element_type=jnp.float32,
        )

    def soften(item, s_ref, p_ref, f_ref, use_mask, live):
        u, t = item // TILES, item % TILES
        if use_mask:
            shift = t * TILE - row_of(u)
            first = jnp.where(live, shift, SEQ * 2)
            last = shift + reach_of(u)
            col = lax.broadcasted_iota(jnp.int32, (STRIP, TILE), 1)
            sink = col < info[4 + u % GROUP] - t * TILE
        for r in range(0, ROWS, STRIP):
            rows = pl.ds(r, STRIP)
            s = s_ref[rows]
            if use_mask:
                gap = gaps[rows]
                s = jnp.where((gap >= first) & ((gap < last) | sink), s, NEG)
            high = jnp.max(s, axis=1, keepdims=True)
            old = top[u, rows]
            new = jnp.maximum(old, high)
            fade = jnp.exp2((old - new) * factor)
            base = new * factor
            part = None
            for n in range(TILE // HD):
                cols = pl.ds(n * HD, HD)
                p = jnp.exp2(s[:, n * HD : (n + 1) * HD] * factor - base)
                p_ref[rows, cols] = p.astype(jnp.bfloat16)
                part = p if part is None else part + p
            tot[u, rows] = tot[u, rows] * fade + part
            top[u, rows] = new
            f_ref[rows] = fade

    def gather_values(item, p_ref, f_ref):
        u = item // TILES
        pv = jnp.dot(p_ref[...], vbuf[span(item % TILES)], preferred_element_type=jnp.float32)
        acc[u] = acc[u] * f_ref[...] + pv

    def run(kind, count, use_mask):
        pb[...] = jnp.zeros_like(pb)
        fb[...] = jnp.ones_like(fb)
        score(items[kind, 0], sa)

        def two(k, before):
            i = 2 * k
            now, then, later = items[kind, i], items[kind, i + 1], items[kind, i + 2]
            score(then, sb)
            gather_values(before, pb, fb)
            soften(now, sa, pa, fa, use_mask, True)
            score(later, sa)
            gather_values(now, pa, fa)
            soften(then, sb, pb, fb, use_mask, i + 1 < count)
            return then

        before = lax.fori_loop(0, (count + 1) // 2, two, items[kind, 0])
        gather_values(before, pb, fb)

    run(0, masked, True)
    run(1, plain, False)

    for u in range(2 * GROUP):
        total = jnp.sum(tot[u], axis=1, keepdims=True)
        out = om if u < GROUP else orr
        j = u % GROUP
        out[:, j * HD : (j + 1) * HD] = (acc[u] / total).astype(jnp.bfloat16)


def attention(info, q_mine, q_other, pieces):
    out = jax.ShapeDtypeStruct((ROWS, GROUP * HD), jnp.bfloat16)
    vmem = pl.BlockSpec(memory_space=pltpu.VMEM)
    state = pltpu.VMEM((2 * GROUP, ROWS, HD), jnp.float32)
    return pl.pallas_call(
        attention_kernel,
        out_shape=(out, out),
        in_specs=[pl.BlockSpec(memory_space=pltpu.SMEM)] + [vmem] * 10,
        out_specs=(vmem, vmem),
        scratch_shapes=[
            pltpu.VMEM((SEQ, HD), jnp.bfloat16),
            pltpu.VMEM((SEQ, HD), jnp.bfloat16),
            pltpu.VMEM((2 * GROUP, ROWS, HD), jnp.bfloat16),
            state,
            state,
            state,
            pltpu.VMEM((ROWS, TILE), jnp.int32),
            pltpu.VMEM((ROWS, TILE), jnp.float32),
            pltpu.VMEM((ROWS, TILE), jnp.float32),
            pltpu.VMEM((ROWS, TILE), jnp.bfloat16),
            pltpu.VMEM((ROWS, TILE), jnp.bfloat16),
            pltpu.VMEM((ROWS, HD), jnp.float32),
            pltpu.VMEM((ROWS, HD), jnp.float32),
            pltpu.SMEM((2, 2 * GROUP * (TILES + 2)), jnp.int32),
        ],
        compiler_params=pltpu.CompilerParams(vmem_limit_bytes=40 * 2**20),
        cost_estimate=pl.CostEstimate(
            flops=7_000_000_000, bytes_accessed=8_000_000, transcendentals=14_000_000
        ),
    )(info, q_mine, q_other, *pieces)


def project_kernel(info, a0, a1, a2, b0, b1, b2, w, out):
    h, z = info[14], info[13]
    width = GROUP * HD

    def term(ref, piece, group, kv):
        start = pl.multiple_of((2 * group + kv) * width, width)
        return jnp.dot(piece, w[pl.ds(start, width)], preferred_element_type=jnp.float32)

    total = term(a0, a0[...], h, z)
    total += term(b0, b0[...], h, 1 - z)
    total += term(a1, a1[...], h ^ 1, z)
    total += term(b1, b1[...], h ^ 3, 1 - z)
    total += term(a2, a2[0], h ^ 3, z)
    total += term(a2, a2[1], h ^ 2, z)
    total += term(b2, b2[0], h ^ 1, 1 - z)
    total += term(b2, b2[1], h ^ 2, 1 - z)
    out[...] = total.astype(out.dtype)


def project(info, pieces, w):
    vmem = pl.BlockSpec(memory_space=pltpu.VMEM)
    return pl.pallas_call(
        project_kernel,
        out_shape=jax.ShapeDtypeStruct((ROWS, w.shape[1]), jnp.bfloat16),
        in_specs=[pl.BlockSpec(memory_space=pltpu.SMEM)] + [vmem] * 7,
        out_specs=vmem,
        compiler_params=pltpu.CompilerParams(vmem_limit_bytes=24 * 2**20),
    )(info, *pieces, w)


def body(queries, keys, values, retrieval, spans, out_weight):
    at = lax.axis_index("ctx")
    h = lax.axis_index("head")
    half, pos = at // 32, at % 32
    width = GROUP * HD
    core = at % 2
    kv_both = jnp.stack([keys, values])
    kv_a = swap(lax.dynamic_slice_in_dim(kv_both, core * HD, HD, axis=2), to_class(0))
    kv_b = swap(lax.dynamic_slice_in_dim(kv_both, (1 - core) * HD, HD, axis=2), to_class(1))
    q_mine = lax.dynamic_slice_in_dim(queries, half * width, width, axis=1)
    q_out = lax.dynamic_slice_in_dim(queries, (1 - half) * width, width, axis=1)
    q_in = swap(q_out, MIRROR)
    first = (2 * h + half) * GROUP
    mine = lambda a: lax.dynamic_slice_in_dim(a, first, GROUP)
    info = jnp.concatenate(
        [
            mine(retrieval),
            mine(spans[0]),
            mine(spans[1]),
            jnp.stack([pos, half, h, jnp.int32(0)]),
        ]
    )
    k = jnp.stack([kv_a[0], kv_b[0]])
    v = jnp.stack([kv_a[1], kv_b[1]])
    for step in range(3):
        if step == 2:
            k, v, q_in = lax.optimization_barrier((k, v, q_in))
        k_got, v_got = swap(k, KEY_STEPS[step]), swap(v, VALUE_STEPS[step])
        k, v = jnp.concatenate([k, k_got]), jnp.concatenate([v, v_got])
    k_last, v_last = swap(k, KEY_STEPS[3]), swap(v, VALUE_STEPS[3])
    pieces = (k, k_last, swap(k, CORE), swap(k_last, CORE))
    pieces += (v, v_last, swap(v, CORE), swap(v_last, CORE))
    att_mine, att_other = attention(info, q_mine, q_in, pieces)

    partner = swap(att_other, MIRROR)
    a1 = lax.ppermute(att_mine, "head", H1)
    b1 = lax.ppermute(partner, "head", H3)
    a2 = lax.ppermute(jnp.stack([att_mine, a1]), "head", H3)
    b2 = lax.ppermute(jnp.stack([partner, b1]), "head", H1)
    return project(info, (att_mine, a1, a2, partner, b1, b2), out_weight)


def solution(mesh):
    in_specs = (P("ctx", "head"), P("ctx", "head"), P("ctx", "head"), P(), P(), P(None, "head"))
    out_specs = P("ctx", "head")
    return jax.shard_map(body, mesh=mesh, in_specs=in_specs, out_specs=out_specs, check_vma=False)
```

```python
import functools

import jax
import jax.numpy as jnp
from jax import lax
from jax.experimental import pallas as pl
from jax.experimental.pallas import tpu as pltpu
from jax.sharding import PartitionSpec as P

HD = 128
ROWS = 192
SEQ = 12288
TILE = 768
TILES = SEQ // TILE
STRIP = 32
GROUP = 4
NEG = -1e30


def ctx_pairs(flip):
    return [(i, i ^ flip) for i in range(64)]


def by_core(flip0, flip1):
    return [(i, i ^ (flip1 if i % 2 else flip0)) for i in range(64)]


def to_class(turn):
    return [(i, ((i % 2) ^ turn) * 32 + (i % 32) // 2 * 2 + i // 32) for i in range(64)]


CORE = ctx_pairs(1)
MIRROR = ctx_pairs(63)
KEY_STEPS = (by_core(2, 8), by_core(6, 24), by_core(8, 2), by_core(24, 6))
VALUE_STEPS = (KEY_STEPS[1], KEY_STEPS[0], KEY_STEPS[3], KEY_STEPS[2])


def head_pairs(flip0, flip1):
    flip = lambda i: flip1 if (i // 4) % 2 else flip0
    return [(i, i ^ flip(i)) for i in range(256)]


HEAD_STEPS = (head_pairs(1, 3), head_pairs(3, 1))


def swap(a, pairs):
    return lax.ppermute(a, "ctx", pairs)


def attention_kernel(retrieval, spans, qm, qr, *refs):
    pieces, (om, orr), scratch = refs[:8], refs[8:10], refs[10:]
    kbuf, vbuf, qbuf, acc, top, tot, gaps, sa, sb, pa, pb, fa, fb, items = scratch
    at = lax.axis_index("ctx")
    half, pos = at // 32, at % 32
    first_head = (2 * lax.axis_index("head") + half) * GROUP
    y, x, core = pos // 8, (pos // 2) % 4, pos % 2

    for s in range(8):
        value, other, late = s // 4, (s // 2) % 2, s % 2
        dst = vbuf if value else kbuf
        f1, f3 = (3, 1) if value else (1, 3)
        z = core ^ other
        for e in range(16):
            a = (f1 * ((e // 2) % 2)) ^ (f3 * ((e // 4) % 2))
            b = (f1 * (e // 8)) ^ (f3 * late)
            fx, fy = jnp.where(z == 0, a, b), jnp.where(z == 0, b, a)
            block = z * 32 + (y ^ fy) * 8 + (x ^ fx) * 2 + (half ^ (e % 2))
            dst[pl.ds(pl.multiple_of(block * ROWS, ROWS), ROWS)] = pieces[s][e]
    for j in range(GROUP):
        qbuf[j] = qm[:, j * HD : (j + 1) * HD]
        qbuf[GROUP + j] = qr[:, j * HD : (j + 1) * HD]
    acc[...] = jnp.zeros_like(acc)
    tot[...] = jnp.zeros_like(tot)
    top[...] = jnp.full_like(top, NEG)
    gaps[...] = lax.broadcasted_iota(jnp.int32, gaps.shape, 0) - lax.broadcasted_iota(
        jnp.int32, gaps.shape, 1
    )

    def row_of(u):
        return jnp.where(u // GROUP == 1, 63 - at, at) * ROWS

    def reach_of(u):
        j = first_head + u % GROUP
        return jnp.where(retrieval[j] > 0, SEQ + ROWS, spans[1, j])

    def list_unit(u, counts):
        row0, reach = row_of(u), reach_of(u)
        low = jnp.maximum(row0 - reach + 1, 0) // TILE
        diag = row0 // TILE

        def put(t, counts):
            edge = (t == diag) | (t * TILE < row0 + ROWS - reach)
            kind = jnp.where(edge, 0, 1)
            n = jnp.where(edge, counts[0], counts[1])
            items[kind, n] = u * TILES + t
            return counts[0] + 1 - kind, counts[1] + kind

        counts = lax.cond(low > 0, lambda c: put(0, c), lambda c: c, counts)
        return lax.fori_loop(low, diag + 1, put, counts)

    masked, plain = lax.fori_loop(0, 2 * GROUP, list_unit, (0, 0))
    odd = plain % 2
    items[0, masked] = items[1, jnp.maximum(plain - 1, 0)]
    masked, plain = masked + odd, plain - odd
    items[0, masked] = items[0, 0]
    items[0, masked + 1] = items[0, 0]
    items[1, plain] = 0

    factor = HD ** (-0.5) * 1.4426950408889634

    def span(t):
        return pl.ds(pl.multiple_of(t * TILE, TILE), TILE)

    def score(item, s_ref):
        s_ref[...] = lax.dot_general(
            qbuf[item // TILES],
            kbuf[span(item % TILES)],
            (((1,), (1,)), ((), ())),
            preferred_element_type=jnp.float32,
        )

    def soften(item, s_ref, p_ref, f_ref, use_mask, live):
        u, t = item // TILES, item % TILES
        if use_mask:
            shift = t * TILE - row_of(u)
            first = jnp.where(live, shift, SEQ * 2)
            last = shift + reach_of(u)
            col = lax.broadcasted_iota(jnp.int32, (STRIP, TILE), 1)
            sink = col < spans[0, first_head + u % GROUP] - t * TILE
        for r in range(0, ROWS, STRIP):
            rows = pl.ds(r, STRIP)
            s = s_ref[rows]
            if use_mask:
                gap = gaps[rows]
                s = jnp.where((gap >= first) & ((gap < last) | sink), s, NEG)
            high = jnp.max(s, axis=1, keepdims=True)
            old = top[u, rows]
            new = jnp.maximum(old, high)
            fade = jnp.exp2((old - new) * factor)
            base = new * factor
            part = None
            for n in range(TILE // HD):
                cols = pl.ds(n * HD, HD)
                p = jnp.exp2(s[:, n * HD : (n + 1) * HD] * factor - base)
                p_ref[rows, cols] = p.astype(jnp.bfloat16)
                part = p if part is None else part + p
            tot[u, rows] = tot[u, rows] * fade + part
            top[u, rows] = new
            f_ref[rows] = fade

    def gather_values(item, p_ref, f_ref):
        u = item // TILES
        pv = jnp.dot(p_ref[...], vbuf[span(item % TILES)], preferred_element_type=jnp.float32)
        acc[u] = acc[u] * f_ref[...] + pv

    def run(kind, count, use_mask):
        pb[...] = jnp.zeros_like(pb)
        fb[...] = jnp.ones_like(fb)
        score(items[kind, 0], sa)

        def two(k, before):
            i = 2 * k
            now, then, later = items[kind, i], items[kind, i + 1], items[kind, i + 2]
            score(then, sb)
            gather_values(before, pb, fb)
            soften(now, sa, pa, fa, use_mask, True)
            score(later, sa)
            gather_values(now, pa, fa)
            soften(then, sb, pb, fb, use_mask, i + 1 < count)
            return then

        before = lax.fori_loop(0, (count + 1) // 2, two, items[kind, 0])
        gather_values(before, pb, fb)

    run(0, masked, True)
    run(1, plain, False)

    for u in range(2 * GROUP):
        total = jnp.sum(tot[u], axis=1, keepdims=True)
        out = om if u < GROUP else orr
        j = u % GROUP
        out[:, j * HD : (j + 1) * HD] = (acc[u] / total).astype(jnp.bfloat16)


def attention(retrieval, spans, q_mine, q_other, pieces):
    out = jax.ShapeDtypeStruct((ROWS, GROUP * HD), jnp.bfloat16)
    vmem = pl.BlockSpec(memory_space=pltpu.VMEM)
    state = pltpu.VMEM((2 * GROUP, ROWS, HD), jnp.float32)
    return pl.pallas_call(
        attention_kernel,
        out_shape=(out, out),
        in_specs=[pl.BlockSpec(memory_space=pltpu.SMEM)] * 2 + [vmem] * 10,
        out_specs=(vmem, vmem),
        scratch_shapes=[
            pltpu.VMEM((SEQ, HD), jnp.bfloat16),
            pltpu.VMEM((SEQ, HD), jnp.bfloat16),
            pltpu.VMEM((2 * GROUP, ROWS, HD), jnp.bfloat16),
            state,
            state,
            state,
            pltpu.VMEM((ROWS, TILE), jnp.int32),
            pltpu.VMEM((ROWS, TILE), jnp.float32),
            pltpu.VMEM((ROWS, TILE), jnp.float32),
            pltpu.VMEM((ROWS, TILE), jnp.bfloat16),
            pltpu.VMEM((ROWS, TILE), jnp.bfloat16),
            pltpu.VMEM((ROWS, HD), jnp.float32),
            pltpu.VMEM((ROWS, HD), jnp.float32),
            pltpu.SMEM((2, 2 * GROUP * (TILES + 2)), jnp.int32),
        ],
        compiler_params=pltpu.CompilerParams(vmem_limit_bytes=20 * 2**20),
        cost_estimate=pl.CostEstimate(
            flops=7_000_000_000, bytes_accessed=8_000_000, transcendentals=14_000_000
        ),
    )(retrieval, spans, q_mine, q_other, *pieces)


def project_kernel(flips, *refs):
    pieces, w, before, out = refs[0], refs[1], refs[2:-1], refs[-1]
    width = GROUP * HD
    h, at = lax.axis_index("head"), lax.axis_index("ctx")
    total = before[0][...] if before else None
    for n, (flip0, flip1) in enumerate(flips):
        group = 2 * (h ^ jnp.where(at % 2 == 0, flip0, flip1))
        for part in range(2):
            kv = group + ((at // 32) ^ part)
            rows = w[pl.ds(pl.multiple_of(kv * width, width), width)]
            term = jnp.dot(pieces[2 * n + part], rows, preferred_element_type=jnp.float32)
            total = term if total is None else total + term
    out[...] = total.astype(out.dtype)


def project(flips, dtype, pieces, w, *before):
    vmem = pl.BlockSpec(memory_space=pltpu.VMEM)
    return pl.pallas_call(
        functools.partial(project_kernel, flips),
        out_shape=jax.ShapeDtypeStruct((ROWS, w.shape[1]), dtype),
        in_specs=[vmem] * (2 + len(before)),
        out_specs=vmem,
        compiler_params=pltpu.CompilerParams(vmem_limit_bytes=16 * 2**20),
        cost_estimate=pl.CostEstimate(
            flops=400_000_000 * len(flips) * 2, bytes_accessed=4_000_000, transcendentals=0
        ),
    )(pieces, w, *before)


def body(queries, keys, values, retrieval, spans, out_weight):
    at = lax.axis_index("ctx")
    half = at // 32
    width = GROUP * HD
    core = at % 2
    kv_both = jnp.stack([keys, values])
    kv_a = swap(lax.dynamic_slice_in_dim(kv_both, core * HD, HD, axis=2), to_class(0))
    kv_b = swap(lax.dynamic_slice_in_dim(kv_both, (1 - core) * HD, HD, axis=2), to_class(1))
    q_mine = lax.dynamic_slice_in_dim(queries, half * width, width, axis=1)
    q_out = lax.dynamic_slice_in_dim(queries, (1 - half) * width, width, axis=1)
    q_in = swap(q_out, MIRROR)
    k = jnp.stack([kv_a[0], kv_b[0]])
    v = jnp.stack([kv_a[1], kv_b[1]])
    for step in range(3):
        k_got, v_got = swap(k, KEY_STEPS[step]), swap(v, VALUE_STEPS[step])
        k, v = jnp.concatenate([k, k_got]), jnp.concatenate([v, v_got])
    k, v, q_in = lax.optimization_barrier((k, v, q_in))
    k_last, v_last = swap(k, KEY_STEPS[3]), swap(v, VALUE_STEPS[3])
    pieces = (k, k_last, swap(k, CORE), swap(k_last, CORE))
    pieces += (v, v_last, swap(v, CORE), swap(v_last, CORE))
    att_mine, att_other = attention(retrieval, spans, q_mine, q_in, pieces)

    held = jnp.stack([att_mine, swap(att_other, MIRROR)])
    near = lax.ppermute(held, ("ctx", "head"), HEAD_STEPS[0])
    total = project(((0, 0),), jnp.float32, held, out_weight)
    both = jnp.concatenate([held, near])
    far = lax.ppermute(both, ("ctx", "head"), HEAD_STEPS[1])
    total = project(((1, 3),), jnp.float32, near, out_weight, total)
    return project(((3, 1), (2, 2)), jnp.bfloat16, far, out_weight, total)


def solution(mesh):
    in_specs = (P("ctx", "head"), P("ctx", "head"), P("ctx", "head"), P(), P(), P(None, "head"))
    out_specs = P("ctx", "head")
    return jax.shard_map(body, mesh=mesh, in_specs=in_specs, out_specs=out_specs, check_vma=False)
```

```python
import functools

import jax
import jax.numpy as jnp
from jax import lax
from jax.experimental import pallas as pl
from jax.experimental.pallas import tpu as pltpu
from jax.sharding import PartitionSpec as P


HD = 128
ROWS = 192
SEQ = 12288
TILE = 768
TILES = SEQ // TILE
HEADS = 32
STRIP = 32
GROUP = 4
NEG = -1e30


def ctx_pairs(flip):
    return [(i, i ^ flip) for i in range(64)]


def by_core(flip0, flip1):
    return [(i, i ^ (flip1 if i % 2 else flip0)) for i in range(64)]


def to_class(turn):
    return [(i, ((i % 2) ^ turn) * 32 + (i % 32) // 2 * 2 + i // 32) for i in range(64)]


CORE = ctx_pairs(1)
MIRROR = ctx_pairs(63)
KEY_STEPS = (by_core(2, 8), by_core(6, 24), by_core(8, 2), by_core(24, 6))
VALUE_STEPS = (KEY_STEPS[1], KEY_STEPS[0], KEY_STEPS[3], KEY_STEPS[2])


def head_pairs(flip0, flip1):
    flip = lambda i: flip1 if (i // 4) % 2 else flip0
    return [(i, i ^ flip(i)) for i in range(256)]


HEAD_STEPS = (head_pairs(1, 3), head_pairs(3, 1))


def swap(a, pairs):
    return lax.ppermute(a, "ctx", pairs)


def head_swap(a, step):
    return lax.ppermute(a, ("ctx", "head"), HEAD_STEPS[step])


def attention_kernel(mirrored, table, q_ref, *refs):
    pieces, out, scratch = refs[:8], refs[8], refs[9:]
    kbuf, vbuf, qbuf, acc, top, tot, gaps, sa, sb, pa, pb, fa, fb, items = scratch
    at = lax.axis_index("ctx")
    half, pos = at // 32, at % 32
    first_head = (2 * lax.axis_index("head") + half) * GROUP
    y, x, core = pos // 8, (pos // 2) % 4, pos % 2

    for s in range(8):
        value, other, late = s // 4, (s // 2) % 2, s % 2
        dst = vbuf if value else kbuf
        f1, f3 = (3, 1) if value else (1, 3)
        z = core ^ other
        for e in range(16):
            a = (f1 * ((e // 2) % 2)) ^ (f3 * ((e // 4) % 2))
            b = (f1 * (e // 8)) ^ (f3 * late)
            fx, fy = jnp.where(z == 0, a, b), jnp.where(z == 0, b, a)
            block = z * 32 + (y ^ fy) * 8 + (x ^ fx) * 2 + (half ^ (e % 2))
            dst[pl.ds(pl.multiple_of(block * ROWS, ROWS), ROWS)] = pieces[s][e]
    for j in range(GROUP):
        qbuf[j] = q_ref[:, j * HD : (j + 1) * HD]
    acc[...] = jnp.zeros_like(acc)
    tot[...] = jnp.zeros_like(tot)
    top[...] = jnp.full_like(top, NEG)
    gaps[...] = lax.broadcasted_iota(jnp.int32, gaps.shape, 0) - lax.broadcasted_iota(
        jnp.int32, gaps.shape, 1
    )

    row0 = (63 - at if mirrored else at) * ROWS

    def reach_of(u):
        return jnp.where(table[first_head + u] > 0, SEQ + ROWS, table[2 * HEADS + first_head + u])

    def list_unit(u, counts):
        reach = reach_of(u)
        low = jnp.maximum(row0 - reach + 1, 0) // TILE
        diag = row0 // TILE

        def put(t, counts):
            edge = (t == diag) | (t * TILE < row0 + ROWS - reach)
            kind = jnp.where(edge, 0, 1)
            n = jnp.where(edge, counts[0], counts[1])
            items[kind, n] = u * TILES + t
            return counts[0] + 1 - kind, counts[1] + kind

        counts = lax.cond(low > 0, lambda c: put(0, c), lambda c: c, counts)
        return lax.fori_loop(low, diag + 1, put, counts)

    masked, plain = lax.fori_loop(0, GROUP, list_unit, (0, 0))
    odd = plain % 2
    items[0, masked] = items[1, jnp.maximum(plain - 1, 0)]
    masked, plain = masked + odd, plain - odd
    items[0, masked] = items[0, 0]
    items[0, masked + 1] = items[0, 0]
    items[1, plain] = 0

    factor = HD ** (-0.5) * 1.4426950408889634

    def span(t):
        return pl.ds(pl.multiple_of(t * TILE, TILE), TILE)

    def score(item, s_ref):
        s_ref[...] = lax.dot_general(
            qbuf[item // TILES],
            kbuf[span(item % TILES)],
            (((1,), (1,)), ((), ())),
            preferred_element_type=jnp.float32,
        )

    def soften(item, s_ref, p_ref, f_ref, use_mask, live):
        u, t = item // TILES, item % TILES
        if use_mask:
            shift = t * TILE - row0
            first = jnp.where(live, shift, SEQ * 2)
            last = shift + reach_of(u)
            col = lax.broadcasted_iota(jnp.int32, (STRIP, TILE), 1)
            sink = col < table[HEADS + first_head + u] - t * TILE
        for r in range(0, ROWS, STRIP):
            rows = pl.ds(r, STRIP)
            s = s_ref[rows]
            if use_mask:
                gap = gaps[rows]
                s = jnp.where((gap >= first) & ((gap < last) | sink), s, NEG)
            high = jnp.max(s, axis=1, keepdims=True)
            old = top[u, rows]
            new = jnp.maximum(old, high)
            fade = jnp.exp2((old - new) * factor)
            base = new * factor
            part = None
            for n in range(TILE // HD):
                cols = pl.ds(n * HD, HD)
                p = jnp.exp2(s[:, n * HD : (n + 1) * HD] * factor - base)
                p_ref[rows, cols] = p.astype(jnp.bfloat16)
                part = p if part is None else part + p
            tot[u, rows] = tot[u, rows] * fade + part
            top[u, rows] = new
            f_ref[rows] = fade

    def gather_values(item, p_ref, f_ref):
        u = item // TILES
        pv = jnp.dot(p_ref[...], vbuf[span(item % TILES)], preferred_element_type=jnp.float32)
        acc[u] = acc[u] * f_ref[...] + pv

    def run(kind, count, use_mask):
        pb[...] = jnp.zeros_like(pb)
        fb[...] = jnp.ones_like(fb)
        score(items[kind, 0], sa)

        def two(k, before):
            i = 2 * k
            now, then, later = items[kind, i], items[kind, i + 1], items[kind, i + 2]
            score(then, sb)
            gather_values(before, pb, fb)
            soften(now, sa, pa, fa, use_mask, True)
            score(later, sa)
            gather_values(now, pa, fa)
            soften(then, sb, pb, fb, use_mask, i + 1 < count)
            return then

        before = lax.fori_loop(0, (count + 1) // 2, two, items[kind, 0])
        gather_values(before, pb, fb)

    run(0, masked, True)
    run(1, plain, False)

    for j in range(GROUP):
        total = jnp.sum(tot[j], axis=1, keepdims=True)
        out[:, j * HD : (j + 1) * HD] = (acc[j] / total).astype(jnp.bfloat16)


def attention(mirrored, table, q, pieces):
    out = jax.ShapeDtypeStruct((ROWS, GROUP * HD), jnp.bfloat16)
    vmem = pl.BlockSpec(memory_space=pltpu.VMEM)
    state = pltpu.VMEM((GROUP, ROWS, HD), jnp.float32)
    return pl.pallas_call(
        functools.partial(attention_kernel, mirrored),
        out_shape=out,
        in_specs=[pl.BlockSpec(memory_space=pltpu.SMEM)] + [vmem] * 9,
        out_specs=vmem,
        scratch_shapes=[
            pltpu.VMEM((SEQ, HD), jnp.bfloat16),
            pltpu.VMEM((SEQ, HD), jnp.bfloat16),
            pltpu.VMEM((GROUP, ROWS, HD), jnp.bfloat16),
            state,
            state,
            state,
            pltpu.VMEM((ROWS, TILE), jnp.int32),
            pltpu.VMEM((ROWS, TILE), jnp.float32),
            pltpu.VMEM((ROWS, TILE), jnp.float32),
            pltpu.VMEM((ROWS, TILE), jnp.bfloat16),
            pltpu.VMEM((ROWS, TILE), jnp.bfloat16),
            pltpu.VMEM((ROWS, HD), jnp.float32),
            pltpu.VMEM((ROWS, HD), jnp.float32),
            pltpu.SMEM((2, GROUP * (TILES + 2)), jnp.int32),
        ],
        compiler_params=pltpu.CompilerParams(vmem_limit_bytes=20 * 2**20),
        cost_estimate=pl.CostEstimate(
            flops=4_000_000_000, bytes_accessed=8_000_000, transcendentals=7_000_000
        ),
    )(table, q, *pieces)


def project_kernel(sources, *refs):
    pieces, w, before, out = refs[: len(sources)], refs[len(sources)], refs[len(sources) + 1 : -1], refs[-1]
    width = GROUP * HD
    h, at = lax.axis_index("head"), lax.axis_index("ctx")
    total = before[0][...] if before else None
    for piece, (part, flips) in zip(pieces, sources):
        for n, (flip0, flip1) in enumerate(flips):
            group = h ^ jnp.where(at % 2 == 0, flip0, flip1)
            start = (2 * group + ((at // 32) ^ part)) * width
            rows = w[pl.ds(pl.multiple_of(start, width), width)]
            value = piece[n] if len(flips) > 1 else piece[...]
            term = jnp.dot(value, rows, preferred_element_type=jnp.float32)
            total = term if total is None else total + term
    out[...] = total.astype(out.dtype)


def project(sources, dtype, pieces, w, *before):
    vmem = pl.BlockSpec(memory_space=pltpu.VMEM)
    count = sum(len(flips) for _, flips in sources)
    return pl.pallas_call(
        functools.partial(project_kernel, sources),
        out_shape=jax.ShapeDtypeStruct((ROWS, w.shape[1]), dtype),
        in_specs=[vmem] * (len(pieces) + 1 + len(before)),
        out_specs=vmem,
        compiler_params=pltpu.CompilerParams(vmem_limit_bytes=16 * 2**20),
        cost_estimate=pl.CostEstimate(
            flops=200_000_000 * count, bytes_accessed=2_000_000 * count, transcendentals=0
        ),
    )(*pieces, w, *before)


SAME, NEAR, FAR = ((0, 0),), ((1, 3),), ((3, 1), (2, 2))


def layer(queries, keys, values, retrieval, spans, out_weight):
    at = lax.axis_index("ctx")
    half = at // 32
    width = GROUP * HD
    core = at % 2
    kv_both = jnp.stack([keys, values])
    kv_a = swap(lax.dynamic_slice_in_dim(kv_both, core * HD, HD, axis=2), to_class(0))
    kv_b = swap(lax.dynamic_slice_in_dim(kv_both, (1 - core) * HD, HD, axis=2), to_class(1))
    q_mine = lax.dynamic_slice_in_dim(queries, half * width, width, axis=1)
    q_out = lax.dynamic_slice_in_dim(queries, (1 - half) * width, width, axis=1)
    k = jnp.stack([kv_a[0], kv_b[0]])
    v = jnp.stack([kv_a[1], kv_b[1]])
    for step in range(3):
        k_got, v_got = swap(k, KEY_STEPS[step]), swap(v, VALUE_STEPS[step])
        k, v = jnp.concatenate([k, k_got]), jnp.concatenate([v, v_got])
    table = jnp.concatenate([retrieval, spans[0], spans[1]])
    k, v, table, q_out = lax.optimization_barrier((k, v, table, q_out))
    k_last, v_last = swap(k, KEY_STEPS[3]), swap(v, VALUE_STEPS[3])
    q_in = swap(q_out, MIRROR)
    pieces = (k, k_last, swap(k, CORE), swap(k_last, CORE))
    pieces += (v, v_last, swap(v, CORE), swap(v_last, CORE))
    mine = attention(False, table, q_mine, pieces)
    mine_near = head_swap(mine, 0)
    q_in, _ = lax.optimization_barrier((q_in, mine))
    other = attention(True, table, q_in, pieces)
    theirs = swap(other, MIRROR)
    mine_far = head_swap(jnp.stack([mine, mine_near]), 1)
    total = project(((0, SAME), (0, NEAR)), jnp.float32, (mine, mine_near), out_weight)
    their_near = head_swap(theirs, 0)
    their_far = head_swap(jnp.stack([theirs, their_near]), 1)
    total = project(((0, FAR), (1, SAME)), jnp.float32, (mine_far, theirs), out_weight, total)
    return project(
        ((1, NEAR), (1, FAR)), jnp.bfloat16, (their_near, their_far), out_weight, total
    )


def solution(mesh):
    in_specs = (P("ctx", "head"), P("ctx", "head"), P("ctx", "head"), P(), P(), P(None, "head"))
    out_specs = P("ctx", "head")
    return jax.shard_map(layer, mesh=mesh, in_specs=in_specs, out_specs=out_specs, check_vma=False)
```

```python
import functools

import jax
import jax.numpy as jnp
from jax import lax
from jax.experimental import pallas as pl
from jax.experimental.pallas import tpu as pltpu
from jax.sharding import PartitionSpec as P


HD = 128
ROWS = 192
SEQ = 12288
TILE = 768
TILES = SEQ // TILE
HEADS = 32
STRIP = 32
UNROLL = 4
GROUP = 4
NEG = -1e30


def ctx_pairs(flip):
    return [(i, i ^ flip) for i in range(64)]


def by_core(flip0, flip1):
    return [(i, i ^ (flip1 if i % 2 else flip0)) for i in range(64)]


def to_class(turn):
    return [(i, ((i % 2) ^ turn) * 32 + (i % 32) // 2 * 2 + i // 32) for i in range(64)]


CORE = ctx_pairs(1)
MIRROR = ctx_pairs(63)
KEY_STEPS = (by_core(2, 8), by_core(6, 24), by_core(8, 2), by_core(24, 6))
VALUE_STEPS = (KEY_STEPS[1], KEY_STEPS[0], KEY_STEPS[3], KEY_STEPS[2])


def head_pairs(flip0, flip1):
    flip = lambda i: flip1 if (i // 4) % 2 else flip0
    return [(i, i ^ flip(i)) for i in range(256)]


HEAD_STEPS = (head_pairs(1, 3), head_pairs(3, 1))


def swap(a, pairs):
    return lax.ppermute(a, "ctx", pairs)


def head_swap(a, step):
    return lax.ppermute(a, ("ctx", "head"), HEAD_STEPS[step])


def attention_kernel(mirrored, table, q_ref, *refs):
    pieces, out, scratch = refs[:8], refs[8], refs[9:]
    kbuf, vbuf, qbuf, acc, top, tot, gaps, sa, sb, pa, pb, fa, fb, items = scratch
    at = lax.axis_index("ctx")
    half, pos = at // 32, at % 32
    first_head = (2 * lax.axis_index("head") + half) * GROUP
    y, x, core = pos // 8, (pos // 2) % 4, pos % 2

    for s in range(8):
        value, other, late = s // 4, (s // 2) % 2, s % 2
        dst = vbuf if value else kbuf
        f1, f3 = (3, 1) if value else (1, 3)
        z = core ^ other
        for e in range(16):
            a = (f1 * ((e // 2) % 2)) ^ (f3 * ((e // 4) % 2))
            b = (f1 * (e // 8)) ^ (f3 * late)
            fx, fy = jnp.where(z == 0, a, b), jnp.where(z == 0, b, a)
            block = z * 32 + (y ^ fy) * 8 + (x ^ fx) * 2 + (half ^ (e % 2))
            dst[pl.ds(pl.multiple_of(block * ROWS, ROWS), ROWS)] = pieces[s][e]
    for j in range(GROUP):
        qbuf[j] = q_ref[:, j * HD : (j + 1) * HD]
    acc[...] = jnp.zeros_like(acc)
    tot[...] = jnp.zeros_like(tot)
    top[...] = jnp.full_like(top, NEG)
    gaps[...] = lax.broadcasted_iota(jnp.int32, gaps.shape, 0) - lax.broadcasted_iota(
        jnp.int32, gaps.shape, 1
    )

    row0 = (63 - at if mirrored else at) * ROWS

    def reach_of(u):
        return jnp.where(table[first_head + u] > 0, SEQ + ROWS, table[2 * HEADS + first_head + u])

    def list_unit(u, counts):
        reach = reach_of(u)
        low = jnp.maximum(row0 - reach + 1, 0) // TILE
        diag = row0 // TILE

        def put(t, counts):
            edge = (t == diag) | (t * TILE < row0 + ROWS - reach)
            kind = jnp.where(edge, 0, 1)
            n = jnp.where(edge, counts[0], counts[1])
            items[kind, n] = u * TILES + t
            return counts[0] + 1 - kind, counts[1] + kind

        counts = lax.cond(low > 0, lambda c: put(0, c), lambda c: c, counts)
        return lax.fori_loop(low, diag + 1, put, counts)

    masked, plain = lax.fori_loop(0, GROUP, list_unit, (0, 0))
    left = plain % UNROLL
    for n in range(UNROLL - 1):
        items[0, masked + n] = items[1, jnp.maximum(plain - 1 - n, 0)]
    masked, plain = masked + left, plain - left
    items[0, masked] = items[0, 0]
    items[0, masked + 1] = items[0, 0]
    items[1, plain] = 0

    factor = HD ** (-0.5) * 1.4426950408889634

    def span(t):
        return pl.ds(pl.multiple_of(t * TILE, TILE), TILE)

    def score(item, s_ref):
        s_ref[...] = lax.dot_general(
            qbuf[item // TILES],
            kbuf[span(item % TILES)],
            (((1,), (1,)), ((), ())),
            preferred_element_type=jnp.float32,
        )

    def soften(item, s_ref, p_ref, f_ref, use_mask, live):
        u, t = item // TILES, item % TILES
        if use_mask:
            shift = t * TILE - row0
            first = jnp.where(live, shift, SEQ * 2)
            last = shift + reach_of(u)
            col = lax.broadcasted_iota(jnp.int32, (STRIP, TILE), 1)
            sink = col < table[HEADS + first_head + u] - t * TILE
        for r in range(0, ROWS, STRIP):
            rows = pl.ds(r, STRIP)
            s = s_ref[rows]
            if use_mask:
                gap = gaps[rows]
                s = jnp.where((gap >= first) & ((gap < last) | sink), s, NEG)
            high = jnp.max(s, axis=1, keepdims=True)
            old = top[u, rows]
            new = jnp.maximum(old, high)
            fade = jnp.exp2((old - new) * factor)
            base = new * factor
            part = None
            for n in range(TILE // HD):
                cols = pl.ds(n * HD, HD)
                p = jnp.exp2(s[:, n * HD : (n + 1) * HD] * factor - base)
                p_ref[rows, cols] = p.astype(jnp.bfloat16)
                part = p if part is None else part + p
            tot[u, rows] = tot[u, rows] * fade + part
            top[u, rows] = new
            f_ref[rows] = fade

    def gather_values(item, p_ref, f_ref):
        u = item // TILES
        pv = jnp.dot(p_ref[...], vbuf[span(item % TILES)], preferred_element_type=jnp.float32)
        acc[u] = acc[u] * f_ref[...] + pv

    def run(kind, count, use_mask, unroll):
        pb[...] = jnp.zeros_like(pb)
        fb[...] = jnp.ones_like(fb)
        score(items[kind, 0], sa)

        def some(k, before):
            i = unroll * k
            for n in range(unroll):
                here, there = ((sa, pa, fa), (sb, pb, fb))[:: 1 if n % 2 == 0 else -1]
                now = items[kind, i + n]
                score(items[kind, i + n + 1], there[0])
                gather_values(before, there[1], there[2])
                soften(now, *here, use_mask, True if n == 0 else i + n < count)
                before = now
            return before

        before = lax.fori_loop(0, (count + unroll - 1) // unroll, some, items[kind, 0])
        gather_values(before, pb, fb)

    run(0, masked, True, 2)
    run(1, plain, False, UNROLL)

    for j in range(GROUP):
        total = jnp.sum(tot[j], axis=1, keepdims=True)
        out[:, j * HD : (j + 1) * HD] = (acc[j] / total).astype(jnp.bfloat16)


def attention(mirrored, table, q, pieces):
    out = jax.ShapeDtypeStruct((ROWS, GROUP * HD), jnp.bfloat16)
    vmem = pl.BlockSpec(memory_space=pltpu.VMEM)
    state = pltpu.VMEM((GROUP, ROWS, HD), jnp.float32)
    return pl.pallas_call(
        functools.partial(attention_kernel, mirrored),
        out_shape=out,
        in_specs=[pl.BlockSpec(memory_space=pltpu.SMEM)] + [vmem] * 9,
        out_specs=vmem,
        scratch_shapes=[
            pltpu.VMEM((SEQ, HD), jnp.bfloat16),
            pltpu.VMEM((SEQ, HD), jnp.bfloat16),
            pltpu.VMEM((GROUP, ROWS, HD), jnp.bfloat16),
            state,
            state,
            state,
            pltpu.VMEM((ROWS, TILE), jnp.int32),
            pltpu.VMEM((ROWS, TILE), jnp.float32),
            pltpu.VMEM((ROWS, TILE), jnp.float32),
            pltpu.VMEM((ROWS, TILE), jnp.bfloat16),
            pltpu.VMEM((ROWS, TILE), jnp.bfloat16),
            pltpu.VMEM((ROWS, HD), jnp.float32),
            pltpu.VMEM((ROWS, HD), jnp.float32),
            pltpu.SMEM((2, GROUP * (TILES + 2)), jnp.int32),
        ],
        compiler_params=pltpu.CompilerParams(vmem_limit_bytes=20 * 2**20),
        cost_estimate=pl.CostEstimate(
            flops=4_000_000_000, bytes_accessed=8_000_000, transcendentals=7_000_000
        ),
    )(table, q, *pieces)


def project_kernel(sources, *refs):
    pieces, w, before, out = refs[: len(sources)], refs[len(sources)], refs[len(sources) + 1 : -1], refs[-1]
    width = GROUP * HD
    h, at = lax.axis_index("head"), lax.axis_index("ctx")
    total = before[0][...] if before else None
    for piece, (part, flips) in zip(pieces, sources):
        for n, (flip0, flip1) in enumerate(flips):
            group = h ^ jnp.where(at % 2 == 0, flip0, flip1)
            start = (2 * group + ((at // 32) ^ part)) * width
            rows = w[pl.ds(pl.multiple_of(start, width), width)]
            value = piece[n] if len(flips) > 1 else piece[...]
            term = jnp.dot(value, rows, preferred_element_type=jnp.float32)
            total = term if total is None else total + term
    out[...] = total.astype(out.dtype)


def project(sources, dtype, pieces, w, *before):
    vmem = pl.BlockSpec(memory_space=pltpu.VMEM)
    count = sum(len(flips) for _, flips in sources)
    return pl.pallas_call(
        functools.partial(project_kernel, sources),
        out_shape=jax.ShapeDtypeStruct((ROWS, w.shape[1]), dtype),
        in_specs=[vmem] * (len(pieces) + 1 + len(before)),
        out_specs=vmem,
        compiler_params=pltpu.CompilerParams(vmem_limit_bytes=16 * 2**20),
        cost_estimate=pl.CostEstimate(
            flops=200_000_000 * count, bytes_accessed=2_000_000 * count, transcendentals=0
        ),
    )(*pieces, w, *before)


SAME, NEAR, FAR = ((0, 0),), ((1, 3),), ((3, 1), (2, 2))


def layer(queries, keys, values, retrieval, spans, out_weight):
    at = lax.axis_index("ctx")
    half = at // 32
    width = GROUP * HD
    core = at % 2
    kv_both = jnp.stack([keys, values])
    kv_a = swap(lax.dynamic_slice_in_dim(kv_both, core * HD, HD, axis=2), to_class(0))
    kv_b = swap(lax.dynamic_slice_in_dim(kv_both, (1 - core) * HD, HD, axis=2), to_class(1))
    q_mine = lax.dynamic_slice_in_dim(queries, half * width, width, axis=1)
    q_out = lax.dynamic_slice_in_dim(queries, (1 - half) * width, width, axis=1)
    k = jnp.stack([kv_a[0], kv_b[0]])
    v = jnp.stack([kv_a[1], kv_b[1]])
    for step in range(3):
        k_got, v_got = swap(k, KEY_STEPS[step]), swap(v, VALUE_STEPS[step])
        k, v = jnp.concatenate([k, k_got]), jnp.concatenate([v, v_got])
    table = jnp.concatenate([retrieval, spans[0], spans[1]])
    k, v, table, q_out = lax.optimization_barrier((k, v, table, q_out))
    k_last, v_last = swap(k, KEY_STEPS[3]), swap(v, VALUE_STEPS[3])
    q_in = swap(q_out, MIRROR)
    pieces = (k, k_last, swap(k, CORE), swap(k_last, CORE))
    pieces += (v, v_last, swap(v, CORE), swap(v_last, CORE))
    mine = attention(False, table, q_mine, pieces)
    mine_near = head_swap(mine, 0)
    q_in, _ = lax.optimization_barrier((q_in, mine))
    other = attention(True, table, q_in, pieces)
    theirs = swap(other, MIRROR)
    mine_far = head_swap(jnp.stack([mine, mine_near]), 1)
    total = project(((0, SAME), (0, NEAR)), jnp.float32, (mine, mine_near), out_weight)
    their_near = head_swap(theirs, 0)
    their_far = head_swap(jnp.stack([theirs, their_near]), 1)
    total = project(((0, FAR), (1, SAME)), jnp.float32, (mine_far, theirs), out_weight, total)
    return project(
        ((1, NEAR), (1, FAR)), jnp.bfloat16, (their_near, their_far), out_weight, total
    )


def solution(mesh):
    in_specs = (P("ctx", "head"), P("ctx", "head"), P("ctx", "head"), P(), P(), P(None, "head"))
    out_specs = P("ctx", "head")
    return jax.shard_map(layer, mesh=mesh, in_specs=in_specs, out_specs=out_specs, check_vma=False)
```

```python
import functools

import jax
import jax.numpy as jnp
from jax import lax
from jax.experimental import pallas as pl
from jax.experimental.pallas import tpu as pltpu
from jax.sharding import PartitionSpec as P


HD = 128
ROWS = 192
SEQ = 12288
TILE = 768
TILES = SEQ // TILE
HEADS = 32
STRIP = 32
UNROLL = 4
GROUP = 4
NEG = -1e30


def ctx_pairs(flip):
    return [(i, i ^ flip) for i in range(64)]


def by_core(flip0, flip1):
    return [(i, i ^ (flip1 if i % 2 else flip0)) for i in range(64)]


def to_class(turn):
    return [(i, ((i % 2) ^ turn) * 32 + (i % 32) // 2 * 2 + i // 32) for i in range(64)]


CORE = ctx_pairs(1)
MIRROR = ctx_pairs(63)
KEY_STEPS = (by_core(2, 8), by_core(6, 24), by_core(8, 2), by_core(24, 6))
VALUE_STEPS = (KEY_STEPS[1], KEY_STEPS[0], KEY_STEPS[3], KEY_STEPS[2])


def head_pairs(flip0, flip1):
    flip = lambda i: flip1 if (i // 4) % 2 else flip0
    return [(i, i ^ flip(i)) for i in range(256)]


HEAD_STEPS = (head_pairs(1, 3), head_pairs(3, 1))


def swap(a, pairs):
    return lax.ppermute(a, "ctx", pairs)


def head_swap(a, step):
    return lax.ppermute(a, ("ctx", "head"), HEAD_STEPS[step])


def attention_kernel(mirrored, table, q_ref, *refs):
    pieces, out, scratch = refs[:8], refs[8], refs[9:]
    kbuf, vbuf, qbuf, acc, top, tot, gaps, sa, sb, pa, pb, fa, fb, items = scratch
    at = lax.axis_index("ctx")
    half, pos = at // 32, at % 32
    first_head = (2 * lax.axis_index("head") + half) * GROUP
    y, x, core = pos // 8, (pos // 2) % 4, pos % 2

    for s in range(8):
        value, other, late = s // 4, (s // 2) % 2, s % 2
        dst = vbuf if value else kbuf
        f1, f3 = (3, 1) if value else (1, 3)
        z = core ^ other
        for e in range(16):
            a = (f1 * ((e // 2) % 2)) ^ (f3 * ((e // 4) % 2))
            b = (f1 * (e // 8)) ^ (f3 * late)
            fx, fy = jnp.where(z == 0, a, b), jnp.where(z == 0, b, a)
            block = z * 32 + (y ^ fy) * 8 + (x ^ fx) * 2 + (half ^ (e % 2))
            dst[pl.ds(pl.multiple_of(block * ROWS, ROWS), ROWS)] = pieces[s][e]
    for j in range(GROUP):
        qbuf[j] = q_ref[:, j * HD : (j + 1) * HD]
    acc[...] = jnp.zeros_like(acc)
    tot[...] = jnp.zeros_like(tot)
    top[...] = jnp.full_like(top, NEG)
    gaps[...] = lax.broadcasted_iota(jnp.int32, gaps.shape, 0) - lax.broadcasted_iota(
        jnp.int32, gaps.shape, 1
    )

    row0 = (63 - at if mirrored else at) * ROWS

    def reach_of(u):
        return jnp.where(table[first_head + u] > 0, SEQ + ROWS, table[2 * HEADS + first_head + u])

    def list_unit(u, counts):
        reach = reach_of(u)
        low = jnp.maximum(row0 - reach + 1, 0) // TILE
        diag = row0 // TILE

        def put(t, counts):
            edge = (t == diag) | (t * TILE < row0 + ROWS - reach)
            kind = jnp.where(edge, 0, 1)
            n = jnp.where(edge, counts[0], counts[1])
            items[kind, n] = u * TILES + t
            return counts[0] + 1 - kind, counts[1] + kind

        counts = lax.cond(low > 0, lambda c: put(0, c), lambda c: c, counts)
        return lax.fori_loop(low, diag + 1, put, counts)

    masked, plain = lax.fori_loop(0, GROUP, list_unit, (0, 0))
    left = plain % UNROLL
    for n in range(UNROLL - 1):
        items[0, masked + n] = items[1, jnp.maximum(plain - 1 - n, 0)]
    masked, plain = masked + left, plain - left
    items[0, masked] = items[0, 0]
    items[0, masked + 1] = items[0, 0]
    items[1, plain] = 0

    factor = HD ** (-0.5) * 1.4426950408889634

    def span(t):
        return pl.ds(pl.multiple_of(t * TILE, TILE), TILE)

    def score(item, s_ref):
        s_ref[...] = lax.dot_general(
            qbuf[item // TILES],
            kbuf[span(item % TILES)],
            (((1,), (1,)), ((), ())),
            preferred_element_type=jnp.float32,
        )

    def soften(item, s_ref, p_ref, f_ref, use_mask, live):
        u, t = item // TILES, item % TILES
        if use_mask:
            shift = t * TILE - row0
            first = jnp.where(live, shift, SEQ * 2)
            last = shift + reach_of(u)
            col = lax.broadcasted_iota(jnp.int32, (STRIP, TILE), 1)
            sink = col < table[HEADS + first_head + u] - t * TILE
        for r in range(0, ROWS, STRIP):
            rows = pl.ds(r, STRIP)
            s = s_ref[rows]
            if use_mask:
                gap = gaps[rows]
                s = jnp.where((gap >= first) & ((gap < last) | sink), s, NEG)
            high = jnp.max(s, axis=1, keepdims=True)
            old = top[u, rows]
            new = jnp.maximum(old, high)
            fade = jnp.exp2((old - new) * factor)
            base = new * factor
            part = None
            for n in range(TILE // HD):
                cols = pl.ds(n * HD, HD)
                p = jnp.exp2(s[:, n * HD : (n + 1) * HD] * factor - base)
                p_ref[rows, cols] = p.astype(jnp.bfloat16)
                part = p if part is None else part + p
            tot[u, rows] = tot[u, rows] * fade + part
            top[u, rows] = new
            f_ref[rows] = fade

    def gather_values(item, p_ref, f_ref):
        u = item // TILES
        pv = jnp.dot(p_ref[...], vbuf[span(item % TILES)], preferred_element_type=jnp.float32)
        acc[u] = acc[u] * f_ref[...] + pv

    def run(kind, count, use_mask, unroll):
        pb[...] = jnp.zeros_like(pb)
        fb[...] = jnp.ones_like(fb)
        score(items[kind, 0], sa)

        def some(k, before):
            i = unroll * k
            for n in range(unroll):
                here, there = ((sa, pa, fa), (sb, pb, fb))[:: 1 if n % 2 == 0 else -1]
                now = items[kind, i + n]
                gather_values(before, there[1], there[2])
                score(items[kind, i + n + 1], there[0])
                soften(now, *here, use_mask, True if n == 0 else i + n < count)
                before = now
            return before

        before = lax.fori_loop(0, (count + unroll - 1) // unroll, some, items[kind, 0])
        gather_values(before, pb, fb)

    run(0, masked, True, 2)
    run(1, plain, False, UNROLL)

    for j in range(GROUP):
        total = jnp.sum(tot[j], axis=1, keepdims=True)
        out[:, j * HD : (j + 1) * HD] = (acc[j] / total).astype(jnp.bfloat16)


def attention(mirrored, table, q, pieces):
    out = jax.ShapeDtypeStruct((ROWS, GROUP * HD), jnp.bfloat16)
    vmem = pl.BlockSpec(memory_space=pltpu.VMEM)
    state = pltpu.VMEM((GROUP, ROWS, HD), jnp.float32)
    return pl.pallas_call(
        functools.partial(attention_kernel, mirrored),
        out_shape=out,
        in_specs=[pl.BlockSpec(memory_space=pltpu.SMEM)] + [vmem] * 9,
        out_specs=vmem,
        scratch_shapes=[
            pltpu.VMEM((SEQ, HD), jnp.bfloat16),
            pltpu.VMEM((SEQ, HD), jnp.bfloat16),
            pltpu.VMEM((GROUP, ROWS, HD), jnp.bfloat16),
            state,
            state,
            state,
            pltpu.VMEM((ROWS, TILE), jnp.int32),
            pltpu.VMEM((ROWS, TILE), jnp.float32),
            pltpu.VMEM((ROWS, TILE), jnp.float32),
            pltpu.VMEM((ROWS, TILE), jnp.bfloat16),
            pltpu.VMEM((ROWS, TILE), jnp.bfloat16),
            pltpu.VMEM((ROWS, HD), jnp.float32),
            pltpu.VMEM((ROWS, HD), jnp.float32),
            pltpu.SMEM((2, GROUP * (TILES + 2)), jnp.int32),
        ],
        compiler_params=pltpu.CompilerParams(vmem_limit_bytes=20 * 2**20),
        cost_estimate=pl.CostEstimate(
            flops=4_000_000_000, bytes_accessed=8_000_000, transcendentals=7_000_000
        ),
    )(table, q, *pieces)


def project_kernel(sources, *refs):
    pieces, w, before, out = refs[: len(sources)], refs[len(sources)], refs[len(sources) + 1 : -1], refs[-1]
    width = GROUP * HD
    h, at = lax.axis_index("head"), lax.axis_index("ctx")
    total = before[0][...] if before else None
    for piece, (part, flips) in zip(pieces, sources):
        for n, (flip0, flip1) in enumerate(flips):
            group = h ^ jnp.where(at % 2 == 0, flip0, flip1)
            start = (2 * group + ((at // 32) ^ part)) * width
            rows = w[pl.ds(pl.multiple_of(start, width), width)]
            value = piece[n] if len(flips) > 1 else piece[...]
            term = jnp.dot(value, rows, preferred_element_type=jnp.float32)
            total = term if total is None else total + term
    out[...] = total.astype(out.dtype)


def project(sources, dtype, pieces, w, *before):
    vmem = pl.BlockSpec(memory_space=pltpu.VMEM)
    count = sum(len(flips) for _, flips in sources)
    return pl.pallas_call(
        functools.partial(project_kernel, sources),
        out_shape=jax.ShapeDtypeStruct((ROWS, w.shape[1]), dtype),
        in_specs=[vmem] * (len(pieces) + 1 + len(before)),
        out_specs=vmem,
        compiler_params=pltpu.CompilerParams(vmem_limit_bytes=16 * 2**20),
        cost_estimate=pl.CostEstimate(
            flops=200_000_000 * count, bytes_accessed=2_000_000 * count, transcendentals=0
        ),
    )(*pieces, w, *before)


SAME, NEAR, FAR = ((0, 0),), ((1, 3),), ((3, 1), (2, 2))


def layer(queries, keys, values, retrieval, spans, out_weight):
    at = lax.axis_index("ctx")
    half = at // 32
    width = GROUP * HD
    core = at % 2
    kv_both = jnp.stack([keys, values])
    kv_a = swap(lax.dynamic_slice_in_dim(kv_both, core * HD, HD, axis=2), to_class(0))
    kv_b = swap(lax.dynamic_slice_in_dim(kv_both, (1 - core) * HD, HD, axis=2), to_class(1))
    q_mine = lax.dynamic_slice_in_dim(queries, half * width, width, axis=1)
    q_out = lax.dynamic_slice_in_dim(queries, (1 - half) * width, width, axis=1)
    k = jnp.stack([kv_a[0], kv_b[0]])
    v = jnp.stack([kv_a[1], kv_b[1]])
    for step in range(3):
        k_got, v_got = swap(k, KEY_STEPS[step]), swap(v, VALUE_STEPS[step])
        k, v = jnp.concatenate([k, k_got]), jnp.concatenate([v, v_got])
    table = jnp.concatenate([retrieval, spans[0], spans[1]])
    k, v, table, q_out = lax.optimization_barrier((k, v, table, q_out))
    k_last, v_last = swap(k, KEY_STEPS[3]), swap(v, VALUE_STEPS[3])
    q_in = swap(q_out, MIRROR)
    pieces = (k, k_last, swap(k, CORE), swap(k_last, CORE))
    pieces += (v, v_last, swap(v, CORE), swap(v_last, CORE))
    mine = attention(False, table, q_mine, pieces)
    mine_near = head_swap(mine, 0)
    q_in, _ = lax.optimization_barrier((q_in, mine))
    other = attention(True, table, q_in, pieces)
    theirs = swap(other, MIRROR)
    mine_far = head_swap(jnp.stack([mine, mine_near]), 1)
    total = project(((0, SAME), (0, NEAR)), jnp.float32, (mine, mine_near), out_weight)
    their_near = head_swap(theirs, 0)
    their_far = head_swap(jnp.stack([theirs, their_near]), 1)
    total = project(
        ((0, FAR), (1, SAME), (1, NEAR)),
        jnp.float32,
        (mine_far, theirs, their_near),
        out_weight,
        total,
    )
    return project(((1, FAR),), jnp.bfloat16, (their_far,), out_weight, total)


def solution(mesh):
    in_specs = (P("ctx", "head"), P("ctx", "head"), P("ctx", "head"), P(), P(), P(None, "head"))
    out_specs = P("ctx", "head")
    return jax.shard_map(layer, mesh=mesh, in_specs=in_specs, out_specs=out_specs, check_vma=False)
```
